128 devices in a mesh: rep: 1, dp: 128 (over x, y, z, core).
Axes of the slice: x: 4, y: 4, z: 4, core: 2. Of those that a mesh axis runs over, the one named last changes fastest.
Arguments:
- x: bfloat16 [128, 1024, 896], P(('rep', 'dp'))
- dy: bfloat16 [128, 1024, 896], P(('rep', 'dp'))
- w_gate: bfloat16 [2, 896, 2560], replicated
- w_up: bfloat16 [2, 896, 2560], replicated
- w_down: bfloat16 [2, 2560, 896], replicated
- m_w_gate: float32 [2, 896, 2560], P(None, 'dp')
- m_w_up: float32 [2, 896, 2560], P(None, 'dp')
- m_w_down: float32 [2, 2560, 896], P(None, 'dp')
- v_w_gate: float32 [2, 896, 2560], P(None, 'dp')
- v_w_up: float32 [2, 896, 2560], P(None, 'dp')
- v_w_down: float32 [2, 2560, 896], P(None, 'dp')
Outputs:
- output 1: bfloat16 [2, 896, 2560], P('rep')
- output 2: bfloat16 [2, 896, 2560], P('rep')
- output 3: bfloat16 [2, 2560, 896], P('rep')
- output 4: float32 [2, 896, 2560], P('rep', 'dp')
- output 5: float32 [2, 896, 2560], P('rep', 'dp')
- output 6: float32 [2, 2560, 896], P('rep', 'dp')
- output 7: float32 [2, 896, 2560], P('rep', 'dp')
- output 8: float32 [2, 896, 2560], P('rep', 'dp')
- output 9: float32 [2, 2560, 896], P('rep', 'dp')
All inputs are finite; a program needn't handle non-finite values.
Results may differ from the reference program's by a relative error of at most 0.022.
Values are sent between devices in bfloat16 or wider.
A program may use at most 1.5 GiB of HBM per device.

```python
import jax
import jax.numpy as jnp
from jax import lax

SEQUENCES = 128
TOKENS = 1024
D = 896
FF = 2560
LAYERS = 2
NAMES = ("w_gate", "w_up", "w_down")
SHAPES = {"w_gate": (LAYERS, D, FF), "w_up": (LAYERS, D, FF), "w_down": (LAYERS, FF, D)}


def bump(key, n, height):
    away = (jnp.arange(n, dtype=jnp.int32) - jax.random.randint(key, (), 0, n, jnp.int32)) % n
    return jnp.where(away < n // 8, height, 1.0)


def together(key, own, strength):
    shared = jax.random.normal(key, own.shape[1:], jnp.float32)
    return (own + strength * shared) * lax.rsqrt(1 + strength * strength)


def setup_inputs(seed: int = 0, part: int = 0) -> dict:
    kx, kdy, ka, kb, kz, kf, kh, kl, *keys = jax.random.split(jax.random.key(seed), 8 + 3 * len(NAMES))
    kx, kdy, ka, kb = (jax.random.fold_in(k, part) for k in (kx, kdy, ka, kb))
    kw, km, kv = (keys[i::3] for i in range(3))
    shape = (SEQUENCES, TOKENS, D)
    much_x, much_dy = jax.random.uniform(kz, (2,), jnp.float32, 0.0, 1.0)
    loud = 2.0 ** jax.random.uniform(jax.random.fold_in(kz, 1), (), jnp.float32, -1.0, 2.0)
    layers = 2.0 ** jax.random.uniform(kl, (LAYERS, 1, 1), jnp.float32, -1.0, 1.0)
    x = together(ka, jax.random.normal(kx, shape, jnp.float32), much_x) * bump(kf, D, 4.0)
    dy = together(kb, jax.random.normal(kdy, shape, jnp.float32), much_dy)
    drawn = {"x": x.astype(jnp.bfloat16), "dy": (loud * dy * (SEQUENCES * TOKENS) ** -0.5).astype(jnp.bfloat16)}
    for key, name in zip(kw, NAMES, strict=True):
        w = jax.random.normal(key, SHAPES[name], jnp.float32) * SHAPES[name][1] ** -0.5
        drawn[name] = (w * {"w_gate": 1.0, "w_up": bump(kh, FF, 4.0), "w_down": layers}[name]).astype(jnp.bfloat16)
    for key, name in zip(km, NAMES, strict=True):
        drawn[f"m_{name}"] = 0.1 * jax.random.normal(key, SHAPES[name], jnp.float32)
    for key, name in zip(kv, NAMES, strict=True):
        drawn[f"v_{name}"] = jax.random.uniform(key, SHAPES[name], jnp.float32, 0.005, 0.015)
    return drawn


def matmul(a, w):
    return jnp.dot(a, w, preferred_element_type=jnp.float32).astype(jnp.bfloat16)


def normed(h):
    wide = h.astype(jnp.float32)
    scale = lax.rsqrt(jnp.mean(wide**2, -1, keepdims=True) + 1e-6)
    return (wide * scale).astype(jnp.bfloat16)


def layer(h, w):
    a = normed(h)
    gate = jnp.dot(a, w["w_gate"], preferred_element_type=jnp.float32)
    up = jnp.dot(a, w["w_up"], preferred_element_type=jnp.float32)
    return h + matmul((jax.nn.silu(gate) * up).astype(jnp.bfloat16), w["w_down"])


def adamw(w, m, v, g):
    m = 0.9 * m + 0.1 * g
    v = 0.95 * v + 0.05 * g * g
    step = m * lax.rsqrt(v + 1e-8) + 0.1 * w
    return (w - 0.02 * step).astype(jnp.bfloat16), m, v


def clipped(gradients, sum_of_squares, count):
    factor = jnp.minimum(1.0, 0.5 * lax.rsqrt(sum_of_squares / count + 1e-30))
    return [g * factor for g in gradients]


def stack(weights, h):
    return lax.scan(lambda h, w: (layer(h, w), None), h, weights)[0]


def reference(x, dy, w_gate, w_up, w_down, m_w_gate, m_w_up, m_w_down, v_w_gate, v_w_up, v_w_down):
    weights = dict(zip(NAMES, (w_gate, w_up, w_down), strict=True))

    def take(so_far, sequence):
        h, by_y = sequence
        _, back = jax.vjp(lambda w: stack(w, h), weights)
        return jax.tree.map(lambda total, term: total + term.astype(jnp.float32), so_far, back(by_y)[0]), None

    none_yet = {name: jnp.zeros(w.shape, jnp.float32) for name, w in weights.items()}
    by_weights, _ = lax.scan(take, none_yet, (x, dy))
    gradients = [by_weights[name].astype(jnp.bfloat16).astype(jnp.float32) for name in NAMES]
    gradients = clipped(gradients, sum(jnp.sum(g * g) for g in gradients), sum(g.size for g in gradients))
    new = [
        adamw(w.astype(jnp.float32), m, v, g)
        for w, m, v, g in zip((w_gate, w_up, w_down), (m_w_gate, m_w_up, m_w_down), (v_w_gate, v_w_up, v_w_down), gradients, strict=True)
    ]
    return tuple(one[which] for which in range(3) for one in new)
```

```python
import functools

import jax
import jax.numpy as jnp
from jax import lax
from jax.experimental import pallas as pl
from jax.experimental.pallas import tpu as pltpu
from jax.sharding import PartitionSpec as P

NAMES = ("w_gate", "w_up", "w_down")
F32, BF16 = jnp.float32, jnp.bfloat16
MESH = pl.DeviceIdType.MESH
STRIDE = {"x": 32, "y": 8, "z": 2}
ORDER = (("y", "z", "x"), ("z", "x", "y"), ("x", "y", "z"))
PAD = (8, 8, 32)
ROWS = (7, 7, 20)


def prod(ns):
    out = 1
    for n in ns:
        out *= n
    return out


def add(dst, *srcs):
    *lead, rows, _ = dst.shape
    steps = rows // 16

    def body(i, carry):
        q, index = i // steps, []
        for n in reversed(lead):
            index.append(q % n)
            q = q // n
        row = slice(None) if steps == 1 else pl.ds(pl.multiple_of((i % steps) * 16, 16), 16)
        at = (*reversed(index), row, slice(None))
        total = srcs[0][at].astype(F32)
        for s in srcs[1:]:
            total = total + s[at].astype(F32)
        dst[at] = total.astype(BF16)
        return carry

    lax.fori_loop(0, prod(lead) * steps, body, 0)


def step_kernel(count, *refs):
    it = iter(refs)

    def take(n):
        return [next(it) for _ in range(n)]

    grads = [take(2) for _ in range(3)]
    w_in, m_in, v_in = take(3), take(3), take(3)
    w_out, m_out, v_out = take(3), take(3), take(3)
    A, R0, R1, R2, R3, S3, R4, G, W5, R5, N = (take(3) for _ in range(11))
    T, n1, n2, n3 = take(4)
    p0s, p0r, p0l, p1s, p1r, p2s, p2r, p3s, p3r, nss, nrs, q3s, q3r, q2s, q2r, q1s, q1r, q0s, q0r, q0l = take(20)

    me = lax.axis_index("dp")
    core = me % 2
    co = {d: (me // s) % 4 for d, s in STRIDE.items()}
    partner = me + 1 - 2 * core
    WL = [(w, l) for w in range(3) for l in range(2)]
    started = []

    def near(dim, offset):
        return me + ((co[dim] + offset) % 4 - co[dim]) * STRIDE[dim]

    def remote(src, dst, ssem, rsem, device):
        return pltpu.make_async_remote_copy(
            src_ref=src, dst_ref=dst, send_sem=ssem, recv_sem=rsem, device_id={"dp": device}, device_id_type=MESH
        )

    def send(*args):
        copy = remote(*args)
        copy.start()
        started.append(copy)
        return copy

    def region(w, ref, k, c, half=None):
        if w == 0:
            return ref.at[pl.ds(2 * c, 2), k] if half is None else ref.at[pl.ds(2 * c + half, 1), k]
        if w == 1:
            return ref.at[:, pl.ds(2 * c, 2), k] if half is None else ref.at[pl.ds(2 * half, 2), pl.ds(2 * c, 2), k]
        return ref.at[k, :, c] if half is None else ref.at[k, pl.ds(2 * half, 2), c]

    def half_of(ref, h):
        n = ref.shape[0] // 2
        return ref.at[pl.ds(n * h, n)]

    def part(w, ref, j):
        return ref.at[:, j] if w == 0 else ref.at[j]

    peers = [partner]
    for d, s in STRIDE.items():
        for k in (1, 2, 3):
            other = near(d, k)
            peers += [other, other + 1 - 2 * core]
    barrier = pltpu.get_barrier_semaphore()
    for p in peers:
        pl.semaphore_signal(barrier, inc=1, device_id={"dp": p}, device_id_type=MESH)
    pl.semaphore_wait(barrier, len(peers))

    p0 = {}
    for oi, off in enumerate((2, 1, 3, 0)):
        for w, l in WL:
            k = (co[ORDER[w][0]] + off) % 4
            i = (oi * 3 + w) * 2 + l
            out = send(region(w, grads[w][l], k, 1 - core), R0[w].at[l, k], p0s.at[i], p0r.at[i], partner)
            own = pltpu.make_async_copy(region(w, grads[w][l], k, core), A[w].at[l, k], p0l.at[i])
            own.start()
            p0[off, w, l] = (out, own)

    def arrive(off, w, l):
        out, own = p0[off, w, l]
        own.wait()
        out.wait_recv()

    p1 = {}

    def p1_send(t, w, l, src, dst, offset):
        i = (w * 2 + l) * 6 + t
        p1[t, w, l] = send(src, dst, p1s.at[i], p1r.at[i], near(ORDER[w][0], offset))

    def blocks(w, l, off):
        k = (co[ORDER[w][0]] + off) % 4
        return A[w].at[l, k], R0[w].at[l, k]

    for w, l in WL:
        arrive(2, w, l)
        a, r = blocks(w, l, 2)
        add(a, a, r)
        p1_send(0, w, l, half_of(a, 0), R1[w].at[l, 0], 1)
        p1_send(1, w, l, half_of(a, 1), R1[w].at[l, 1], -1)
    for w, l in WL:
        arrive(1, w, l)
        a, r = (half_of(b, 1) for b in blocks(w, l, 1))
        add(a, a, r)
        p1_send(2, w, l, a, half_of(R2[w].at[l, 0], 1), 1)
        arrive(3, w, l)
        a, r = (half_of(b, 0) for b in blocks(w, l, 3))
        add(a, a, r)
        p1_send(3, w, l, a, half_of(R2[w].at[l, 1], 0), -1)
    for w, l in WL:
        p1[0, w, l].wait_recv()
        a, r = (half_of(b, 0) for b in blocks(w, l, 1))
        add(a, a, r, R1[w].at[l, 0])
        p1_send(4, w, l, a, half_of(R2[w].at[l, 0], 0), 1)
        p1[1, w, l].wait_recv()
        a, r = (half_of(b, 1) for b in blocks(w, l, 3))
        add(a, a, r, R1[w].at[l, 1])
        p1_send(5, w, l, a, half_of(R2[w].at[l, 1], 1), -1)
    p2 = {}
    for w, l in WL:
        arrive(0, w, l)
        for t in (2, 3, 4, 5):
            p1[t, w, l].wait_recv()
        a, r = blocks(w, l, 0)
        add(a, a, r, R2[w].at[l, 0], R2[w].at[l, 1])
        d2 = ORDER[w][1]
        for j in (1, 2, 3):
            i = (w * 2 + l) * 3 + j - 1
            p2[j, w, l] = send(
                part(w, a, (co[d2] + j) % 4), R3[w].at[l, j - 1], p2s.at[i], p2r.at[i], near(d2, j)
            )

    def exchange(w, l, e, c):
        d3 = ORDER[w][2]
        other = me + (2 * core + e - co[d3]) * STRIDE[d3] + c - core
        copy = remote(
            S3[w].at[l, e, c], R4[w].at[l, co[d3]], p3s.at[((w * 2 + l) * 2 + e) * 2 + c], p3r.at[(w * 2 + l) * 4 + co[d3]], other
        )
        return other, copy

    for w, l in WL:
        for j in (1, 2, 3):
            p2[j, w, l].wait_recv()
        own = part(w, blocks(w, l, 0)[0], co[ORDER[w][1]])
        terms = [own] + [R3[w].at[l, j] for j in range(3)]
        if w < 2:
            for e in range(2):
                total = sum((t[e].astype(F32) for t in terms[1:]), terms[0][e].astype(F32))
                for c in range(2):
                    S3[w][l, e, c] = total[8 * c : 8 * c + 8].astype(BF16)
        else:
            for r in range(5):
                rows = slice(16 * r, 16 * r + 16)
                T[rows] = sum((t[rows].astype(F32) for t in terms[1:]), terms[0][rows].astype(F32))
            for e in range(2):
                for c in range(2):
                    piece = T[40 * e + 20 * c : 40 * e + 20 * c + 20]
                    G[2][l, 0:20] = piece
                    G[2][l, 20:32] = jnp.zeros((12, piece.shape[1]), F32)
                    S3[2][l, e, c] = G[2][l].astype(BF16)
        for e in range(2):
            for c in range(2):
                other, copy = exchange(w, l, e, c)

                @pl.when(other != me)
                def _():
                    copy.start()

                @pl.when(other == me)
                def _():
                    R4[w][l, co[ORDER[w][2]]] = S3[w][l, e, c]

    squares = jnp.zeros((8, 128), F32)
    for w, l in WL:
        d3 = ORDER[w][2]
        for s in range(4):
            mine = (co[d3] == s) & (co[d3] // 2 == core)

            @pl.when(jnp.logical_not(mine))
            def _():
                remote(S3[w].at[l, 0, 0], R4[w].at[l, s], p3s.at[0], p3r.at[(w * 2 + l) * 4 + s], me).wait_recv()

        g = sum((R4[w][l, s].astype(F32) for s in range(1, 4)), R4[w][l, 0].astype(F32)).astype(BF16).astype(F32)
        G[w][l] = g
        sq = g * g
        for r in range(0, sq.shape[0], 8):
            for c in range(0, sq.shape[1], 128):
                squares = squares + sq[r : r + 8, c : c + 128]

    line = co["z"] * 2 + core
    n1[line] = squares
    copies = []
    for j in range(1, 8):
        other = me + (line + j) % 8 - line
        copies.append(send(n1.at[line], n1.at[line], nss.at[j - 1], nrs.at[j - 1], other))
    for copy in copies:
        copy.wait_recv()
    for base, ref, dim, before in ((7, n2, "y", n1), (10, n3, "x", n2)):
        total = before[0]
        for s in range(1, before.shape[0]):
            total = total + before[s]
        ref[co[dim]] = total
        copies = []
        for j in (1, 2, 3):
            i = base + j - 1
            copies.append(send(ref.at[co[dim]], ref.at[co[dim]], nss.at[i], nrs.at[i], near(dim, j)))
        for copy in copies:
            copy.wait_recv()
    total = n3[0] + n3[1] + n3[2] + n3[3]
    total = jnp.sum(jnp.sum(total, axis=0, keepdims=True), axis=1, keepdims=True)
    factor = jnp.minimum(1.0, 0.5 * lax.rsqrt(total * (1.0 / count) + 1e-30))

    def spread(w, l, k):
        d3 = ORDER[w][2]
        to = co[d3] // 2
        other = me + (k - co[d3]) * STRIDE[d3] + to - core
        slot = (co[d3] % 2) * 2 + core
        copy = remote(W5[w].at[l], R5[w].at[l, slot], q3s.at[(w * 2 + l) * 4 + k], q3r.at[(w * 2 + l) * 4 + slot], other)
        return other, slot, copy

    for w, l in WL:
        n = ROWS[w]
        g = G[w][l, 0:n] * factor
        m = 0.9 * m_in[w][l] + 0.1 * g
        v = 0.95 * v_in[w][l] + 0.05 * g * g
        m_out[w][l] = m
        v_out[w][l] = v
        old = w_in[w][l]
        G[w][l, 0:n] = old - 0.02 * (m * lax.rsqrt(v + 1e-8) + 0.1 * old)
        W5[w][l] = G[w][l].astype(BF16)
        for k in range(4):
            other, slot, copy = spread(w, l, k)

            @pl.when(other != me)
            def _():
                copy.start()

            @pl.when(other == me)
            def _():
                R5[w][l, slot] = W5[w][l]

    q2 = {}
    for w, l in WL:
        d2, d3 = ORDER[w][1:]
        for s in range(4):
            mine = (co[d3] // 2 == core) & ((co[d3] % 2) * 2 + core == s)

            @pl.when(jnp.logical_not(mine))
            def _():
                remote(W5[w].at[l], R5[w].at[l, s], q3s.at[0], q3r.at[(w * 2 + l) * 4 + s], me).wait_recv()

        block = part(w, N[w].at[l], co[d2])
        if w < 2:
            for e in range(2):
                both = [R5[w][l, 2 * e + c].astype(F32) for c in range(2)]
                block[e] = jnp.concatenate(both, axis=0).astype(BF16)
        else:
            for s in range(4):
                T[20 * s : 20 * s + 20] = R5[w][l, s].astype(F32)[0:20]
            for r in range(5):
                block[16 * r : 16 * r + 16] = T[16 * r : 16 * r + 16].astype(BF16)
        for j in (1, 2, 3):
            i = (w * 2 + l) * 3 + j - 1
            q2[j, w, l] = send(block, block, q2s.at[i], q2r.at[i], near(d2, j))

    q1, q0, local = {}, {}, []

    def q1_send(t, w, l, src, dst, offset):
        i = (w * 2 + l) * 4 + t
        q1[t, w, l] = send(src, dst, q1s.at[i], q1r.at[i], near(ORDER[w][0], offset))

    def q0_send(t, w, l, src, dst):
        i = (w * 2 + l) * 5 + t
        q0[t, w, l] = send(src, dst, q0s.at[i], q0r.at[i], partner)

    for w, l in WL:
        for j in (1, 2, 3):
            q2[j, w, l].wait_recv()
        here = region(w, w_out[w].at[l], co[ORDER[w][0]], core)
        q1_send(0, w, l, N[w].at[l], here, 1)
        q1_send(1, w, l, N[w].at[l], here, -1)
        q0_send(0, w, l, N[w].at[l], here)
        copy = pltpu.make_async_copy(N[w].at[l], here, q0l.at[w * 2 + l])
        copy.start()
        local.append(copy)
    for w, l in WL:
        d1 = ORDER[w][0]
        for t, off, h, to in ((0, 3, 0, 1), (1, 1, 1, -1)):
            q1[t, w, l].wait_recv()
            k = (co[d1] + off) % 4
            half = region(w, w_out[w].at[l], k, core, h)
            q1_send(2 + t, w, l, half, half, to)
            whole = region(w, w_out[w].at[l], k, core)
            q0_send(1 + t, w, l, whole, whole)
    for w, l in WL:
        for t in (0, 1):
            q1[2 + t, w, l].wait_recv()
            half = region(w, w_out[w].at[l], (co[ORDER[w][0]] + 2) % 4, core, t)
            q0_send(3 + t, w, l, half, half)
    for copy in q0.values():
        copy.wait_recv()
    for copy in local:
        copy.wait()
    for copy in started:
        copy.wait_send()
    for w, l in WL:
        for e in range(2):
            for c in range(2):
                other, copy = exchange(w, l, e, c)

                @pl.when(other != me)
                def _():
                    copy.wait_send()

        for k in range(4):
            other, _, copy = spread(w, l, k)

            @pl.when(other != me)
            def _():
                copy.wait_send()


def reduce_and_step(grads, weights, m, v, ff, d, count):
    inner = ((2, 4, 16, ff), (4, 2, 16, ff), (4, 80, d))
    half = ((1, 4, 16, ff), (2, 2, 16, ff), (2, 80, d))
    small = ((2, 16, ff), (2, 16, ff), (80, d))
    width = (ff, ff, d)
    whole = ((2, 4, 4, 4, 16, ff), (2, 4, 4, 4, 16, ff), (2, 4, 4, 2, 80, d))

    def vmem(shapes, dtype=BF16):
        return [pltpu.VMEM(s, dtype) for s in shapes]

    three = range(3)
    scratch = (
        vmem((2, 4, *inner[w]) for w in three)
        + vmem((2, 4, *inner[w]) for w in three)
        + vmem((2, 2, *half[w]) for w in three)
        + vmem((2, 2, *inner[w]) for w in three)
        + vmem((2, 3, *small[w]) for w in three)
        + vmem((2, 2, 2, PAD[w], width[w]) for w in three)
        + vmem((2, 4, PAD[w], width[w]) for w in three)
        + vmem(((2, PAD[w], width[w]) for w in three), F32)
        + vmem((2, PAD[w], width[w]) for w in three)
        + vmem((2, 4, PAD[w], width[w]) for w in three)
        + vmem((2, *inner[w]) for w in three)
        + vmem(((80, d), (8, 8, 128), (4, 8, 128), (4, 8, 128)), F32)
        + [pltpu.SemaphoreType.DMA((n,)) for n in (24, 24, 24, 36, 36, 18, 18, 24, 24, 13, 13, 24, 24, 18, 18, 24, 24, 30, 30, 6)]
    )
    in_vmem, anywhere = pl.BlockSpec(memory_space=pltpu.VMEM), pl.BlockSpec(memory_space=pl.ANY)
    moments = [jax.ShapeDtypeStruct(t.shape, F32) for t in m]
    out = pl.pallas_call(
        functools.partial(step_kernel, count),
        out_shape=[jax.ShapeDtypeStruct(s, BF16) for s in whole] + moments + moments,
        in_specs=[anywhere] * 6 + [in_vmem] * 9,
        out_specs=[anywhere] * 3 + [in_vmem] * 6,
        scratch_shapes=scratch,
        compiler_params=pltpu.CompilerParams(collective_id=0, has_side_effects=True, vmem_limit_bytes=66_000_000),
        name="reduce_and_step",
    )(*(g for pair in grads for g in pair), *weights, *m, *v)
    return out[:3], out[3:6], out[6:]


def matmul(a, w):
    return jnp.dot(a, w, preferred_element_type=F32).astype(BF16)


def to_rows(a, b):
    return lax.dot_general(a, b, (((0,), (0,)), ((), ())), preferred_element_type=F32).astype(BF16)


def times_transposed(a, w):
    return lax.dot_general(a, w, (((1,), (1,)), ((), ())), preferred_element_type=F32).astype(BF16)


def normed(h):
    wide = h.astype(F32)
    scale = lax.rsqrt(jnp.mean(wide**2, -1, keepdims=True) + 1e-6)
    return (wide * scale).astype(BF16)


def gated(gate, up):
    return jax.nn.silu(gate) * up


def gradients_of(x, dy, w_gate, w_up, w_down):
    d = x.shape[1]
    column = lax.broadcasted_iota(jnp.int32, (d, d // 7 * 8), 1)
    row = lax.broadcasted_iota(jnp.int32, (d, d // 7 * 8), 0)
    spread = ((row // 7) * 8 + row % 7 == column).astype(BF16)
    layers = w_gate.shape[0]
    h, saved = x, []
    for n in range(layers):
        a = normed(h)
        gate = jnp.dot(a, w_gate[n], preferred_element_type=F32)
        up = jnp.dot(a, w_up[n], preferred_element_type=F32)
        act = gated(gate, up).astype(BF16)
        saved.append((h, a, gate, up, act))
        if n + 1 < layers:
            h = h + matmul(act, w_down[n])
    grads = [None] * layers
    for n in reversed(range(layers)):
        h, a, gate, up, act = saved[n]
        by_act = times_transposed(dy, w_down[n])
        by_down = to_rows(act, dy)
        _, back = jax.vjp(gated, gate, up)
        by_gate, by_up = (t.astype(BF16) for t in back(by_act.astype(F32)))
        a_spread = matmul(a, spread)
        grads[n] = (to_rows(a_spread, by_gate), to_rows(a_spread, by_up), by_down)
        if n:
            by_a = times_transposed(by_gate, w_gate[n]) + times_transposed(by_up, w_up[n])
            _, back = jax.vjp(normed, h)
            dy = dy + back(by_a)[0]
    return [[grads[n][w] for n in range(layers)] for w in range(3)]


def solution(mesh):
    def step(x, dy, *arrays):
        weights, m, v = (arrays[i : i + 3] for i in (0, 3, 6))
        layers, d, ff = weights[0].shape
        me = lax.axis_index("dp")
        rows = [
            lax.dynamic_slice_in_dim(w, me * n, n, axis=1).astype(F32) for w, n in zip(weights, ROWS, strict=True)
        ]
        grads = gradients_of(x[0], dy[0], *weights)
        shapes = ((4, 4, 4, 16, ff), (4, 4, 4, 16, ff), (4, 4, 2, 80, d))
        grads = [[g.reshape(s) for g in pair] for pair, s in zip(grads, shapes, strict=True)]
        count = sum(w.size for w in weights)
        new, m, v = reduce_and_step(grads, rows, m, v, ff, d, count)
        gate, up = (t.reshape(layers, d // 7, 8, ff)[:, :, :7].reshape(layers, d, ff) for t in new[:2])
        return gate, up, new[2].reshape(layers, ff, d), *m, *v

    whole, cut = P(None, None, None), P(None, "dp", None)
    tokens = P(("rep", "dp"), None, None)
    return jax.shard_map(
        step,
        mesh=mesh,
        in_specs=(tokens, tokens, *[whole] * 3, *[cut] * 6),
        out_specs=(*[P("rep", None, None)] * 3, *[P("rep", "dp", None)] * 6),
        check_vma=False,
    )
```
